32 devices in a mesh: dp: 8 (over z, y), rep: 4 (over x, core).
Axes of the slice: x: 2, y: 2, z: 4, core: 2. Of those that a mesh axis runs over, the one named last changes fastest.
Arguments:
- enc: bfloat16 [64, 48, 640], P(('dp', 'rep')), may hold values from -6 to 6
- pred: bfloat16 [64, 17, 640], P(('dp', 'rep')), may hold values from -6 to 6
- labels: int32 [64, 16], P(('dp', 'rep')), may hold values from 1 to 4095
- frame_len: int32 [64], P(('dp', 'rep')), may hold values from 24 to 48, as said below
- label_len: int32 [64], P(('dp', 'rep')), may hold values from 1 to 16, as said below
- w_enc: bfloat16 [640, 640], replicated, may hold values from -0.25 to 0.25
- w_pred: bfloat16 [640, 640], replicated, may hold values from -0.25 to 0.25
- b_joint: bfloat16 [640], replicated, may hold values from -3 to 3
- w_out: bfloat16 [640, 4096], replicated, may hold values from -0.69921875 to 0.69921875
- b_out: bfloat16 [4096], replicated, may hold values from -5 to 5
Outputs:
- step_enc: float32 [640, 640], replicated
- step_pred: float32 [640, 640], replicated
- step_out: float32 [640, 4096], replicated
- step_bias_out: float32 [4096], replicated
- step_bias_joint: float32 [640], replicated
- mean_loss: float32 [], replicated
The draws below stay inside these ranges and needn't reach their ends.
Inputs may be any that keep to these rules, and one draw needn't show every extreme that they name: `frame_len`: the last utterance has all 48 frames. `label_len`: the last utterance has all 16 labels.
All inputs are finite; a program needn't handle non-finite values.
Results may differ from the reference program's by a relative error of at most 0.0055.
Values sent between devices are 32-bit elements; how exact they have to be, the bound alone decides.
No kernel may reach another device: no remote copies, remote signals or barrier semaphores. Data moves between devices by JAX's collectives and lax.ppermute only.
A program may use at most 256 MiB of HBM per device.

```python
import jax
import jax.numpy as jnp
from jax import lax

ENC_DIM = 640
PRED_DIM = 640
JOINT = 640
VOCAB = 4096
FRAMES = 48
LABELS = 16
BATCH = 64


def draw_frame_len(key, part):
    positions = jnp.arange(BATCH, dtype=jnp.int32)
    picked = jax.random.randint(jax.random.fold_in(key, 11), (BATCH,), FRAMES // 2, FRAMES + 1)
    return jnp.where(positions == BATCH - 1, FRAMES, picked).astype(jnp.int32)


def draw_label_len(key, part):
    positions = jnp.arange(BATCH, dtype=jnp.int32)
    baseline = LABELS * (BATCH + 2 * positions) // (3 * BATCH)
    jitter = jax.random.randint(jax.random.fold_in(key, 23), (BATCH,), -1, 2)
    lengths = jnp.clip(baseline + jitter, 1, LABELS)
    return jnp.where(positions == BATCH - 1, LABELS, lengths).astype(jnp.int32)


def place_ends(drawn, stream_key, least, top_value):
    place = [jax.random.randint(jax.random.fold_in(stream_key, axis), (), 0, length) for axis, length in enumerate(drawn.shape)]
    main_axis = drawn.shape.index(max(drawn.shape))
    neighbour = place[:main_axis] + [(place[main_axis] + 1) % drawn.shape[main_axis]] + place[main_axis + 1:]
    return drawn.at[tuple(place)].set(least).at[tuple(neighbour)].set(top_value)


def level_of(rng, shape, cuts, smallest, high):
    level = 1.0
    for axis_at, shards_of in cuts:
        steps = jax.random.uniform(jax.random.fold_in(jax.random.fold_in(rng, 6), axis_at), (shards_of,), jnp.float32, smallest / len(cuts), high / len(cuts))
        level = level * jnp.repeat(jnp.exp(steps), shape[axis_at] // shards_of).reshape((-1,) + (1,) * (len(shape) - 1 - axis_at))
    return level


def gaussian(stream_key, shape, width, limit, split=(), held_as=jnp.bfloat16):
    factor_of = level_of(stream_key, shape, split, -0.22, 0.18) if split else 1.0
    result = jax.random.normal(stream_key, shape, jnp.float32) * width * factor_of
    return jnp.minimum(jnp.maximum(result, -limit), limit).astype(held_as)


def setup_inputs(seed: int = 0) -> dict:
    seeds = jax.random.split(jax.random.key(seed), 11)
    return {
        "enc": gaussian(seeds[0], (BATCH, FRAMES, ENC_DIM), 1.0, 6.0, ((0, 32),)),
        "pred": gaussian(seeds[1], (BATCH, LABELS + 1, PRED_DIM), 1.0, 6.0, ((0, 32),)),
        "labels": place_ends(jax.random.randint(seeds[2], (BATCH, LABELS), 1, VOCAB), jax.random.fold_in(seeds[2], 1), 1, VOCAB - 1).astype(jnp.int32),
        "frame_len": draw_frame_len(jax.random.fold_in(seeds[10], 71), 0),
        "label_len": draw_label_len(jax.random.fold_in(seeds[10], 71), 0),
        "w_enc": gaussian(seeds[5], (ENC_DIM, JOINT), ENC_DIM ** -0.5, 0.25),
        "w_pred": gaussian(seeds[6], (PRED_DIM, JOINT), PRED_DIM ** -0.5, 0.25),
        "b_joint": gaussian(seeds[7], (JOINT,), 0.5, 3.0),
        "w_out": gaussian(seeds[8], (JOINT, VOCAB), 0.12, 0.69921875),
        "b_out": gaussian(seeds[9], (VOCAB,), 1.0, 5.0),
    }


NEG = -1e+30
EPS = 1e-06

def forward_rows(blank, emit):
    count_labels = blank.shape[1]
    positions = jnp.arange(count_labels, dtype=jnp.int32)

    def along_labels(carry_left, inputs):
        top_term, emit_here = inputs
        cell_value = jnp.logaddexp(top_term, carry_left)
        return (cell_value + emit_here, cell_value)

    def along_frames(top_row, inputs):
        blank_row, emit_row = inputs
        unused_carry, alpha_row = lax.scan(along_labels, jnp.float32(NEG), (top_row, emit_row))
        return (alpha_row + blank_row, alpha_row)
    first_top = jnp.where(positions == 0, 0.0, NEG).astype(jnp.float32)
    unused_last, alpha = lax.scan(along_frames, first_top, (blank, emit))
    return alpha

def backward_rows(blank, emit, frame_count, label_count):
    num_frames, count_labels = blank.shape
    positions = jnp.arange(count_labels, dtype=jnp.int32)
    neg_row = jnp.full((count_labels,), NEG, jnp.float32)
    terminal = jnp.where(positions == label_count, 0.0, NEG).astype(jnp.float32)

    def along_labels_back(carry_right, inputs):
        below_value, blank_here, emit_here, live = inputs
        cell_value = jnp.logaddexp(below_value + blank_here, carry_right + emit_here)
        cell_value = jnp.where(live, cell_value, NEG).astype(jnp.float32)
        return (cell_value, cell_value)

    def along_frames_back(carry_below, inputs):
        frame_pos, blank_row, emit_row = inputs
        below = jnp.where(frame_pos == frame_count - 1, terminal, jnp.where(frame_pos >= frame_count, neg_row, carry_below))
        live = (positions <= label_count) & (frame_pos < frame_count)
        unused_carry, beta_row = lax.scan(along_labels_back, jnp.float32(NEG), (below, blank_row, emit_row, live), reverse=True)
        return (beta_row, (beta_row, below))
    frame_ids = jnp.arange(num_frames, dtype=jnp.int32)
    unused_last, (beta, below) = lax.scan(along_frames_back, neg_row, (frame_ids, blank, emit), reverse=True)
    return (beta, below)

def utterance_terms(enc_row, pred_row, label_row, frame_count, label_count, w_enc, w_pred, b_joint, w_out, b_out):
    num_frames = enc_row.shape[0]
    count_labels = pred_row.shape[0]
    joint_width = w_enc.shape[1]
    vocab_size = w_out.shape[1]
    enc_proj = jnp.dot(enc_row, w_enc, preferred_element_type=jnp.float32)
    pred_proj = jnp.dot(pred_row, w_pred, preferred_element_type=jnp.float32) + b_joint.astype(jnp.float32)
    hidden = jnp.tanh(enc_proj[:, None, :] + pred_proj[None, :, :]).astype(jnp.bfloat16)
    hidden = lax.optimization_barrier(hidden.reshape(num_frames * count_labels, joint_width))
    logits = jnp.dot(hidden, w_out, preferred_element_type=jnp.float32) + b_out.astype(jnp.float32)
    log_probs = jax.nn.log_softmax(logits, axis=-1)
    targets = jnp.concatenate([label_row.astype(jnp.int32), jnp.ones((1,), jnp.int32)])
    target_cols = jnp.tile(targets, num_frames)
    vocab_pos = jnp.arange(vocab_size, dtype=jnp.int32)
    is_target = vocab_pos[None, :] == target_cols[:, None]
    emit = lax.optimization_barrier(jnp.sum(jnp.where(is_target, log_probs, 0.0), axis=1)).reshape(num_frames, count_labels)
    blank = log_probs[:, 0].reshape(num_frames, count_labels)
    alpha = forward_rows(blank, emit)
    beta, below = backward_rows(blank, emit, frame_count, label_count)
    log_total = beta[0, 0]
    right = jnp.concatenate([beta[:, 1:], jnp.full((num_frames, 1), NEG, jnp.float32)], axis=1)
    blank_occ = jnp.exp(alpha + blank + below - log_total).reshape(-1)
    emit_occ = jnp.exp(alpha + emit + right - log_total).reshape(-1)
    probs = jnp.exp(log_probs)
    grad_logits = probs * (blank_occ + emit_occ)[:, None]
    grad_logits = grad_logits - jnp.where(vocab_pos[None, :] == 0, blank_occ[:, None], 0.0)
    grad_logits = grad_logits - jnp.where(is_target, emit_occ[:, None], 0.0)
    grad_logits = lax.optimization_barrier(grad_logits.astype(jnp.bfloat16))
    grad_out = lax.dot_general(hidden, grad_logits, (((0,), (0,)), ((), ())), preferred_element_type=jnp.float32)
    grad_bias_out = lax.optimization_barrier(jnp.sum(grad_logits.astype(jnp.float32), axis=0))
    grad_hidden = lax.dot_general(grad_logits, w_out, (((1,), (1,)), ((), ())), preferred_element_type=jnp.float32)
    hidden_wide = hidden.astype(jnp.float32)
    grad_pre = (grad_hidden * (1.0 - hidden_wide * hidden_wide)).reshape(num_frames, count_labels, joint_width)
    grad_enc_proj = lax.optimization_barrier(lax.optimization_barrier(jnp.sum(grad_pre, axis=1)).astype(jnp.bfloat16))
    grad_pred_proj = lax.optimization_barrier(lax.optimization_barrier(jnp.sum(grad_pre, axis=0)).astype(jnp.bfloat16))
    grad_enc = lax.dot_general(enc_row, grad_enc_proj, (((0,), (0,)), ((), ())), preferred_element_type=jnp.float32)
    grad_pred = lax.dot_general(pred_row, grad_pred_proj, (((0,), (0,)), ((), ())), preferred_element_type=jnp.float32)
    grad_bias_joint = lax.optimization_barrier(jnp.sum(grad_pred_proj.astype(jnp.float32), axis=0))
    return (-log_total, (grad_enc, grad_pred, grad_out, grad_bias_out, grad_bias_joint))

def local_sums(enc, pred, labels, frame_len, label_len, w_enc, w_pred, b_joint, w_out, b_out):
    initial = (jnp.zeros(w_enc.shape, jnp.float32), jnp.zeros(w_pred.shape, jnp.float32), jnp.zeros(w_out.shape, jnp.float32), jnp.zeros(b_out.shape, jnp.float32), jnp.zeros(b_joint.shape, jnp.float32))

    def one_utterance(carry, inputs):
        loss_sum, grad_sums = carry
        enc_row, pred_row, label_row, frame_count, label_count = inputs
        loss_one, grads_one = utterance_terms(enc_row, pred_row, label_row, frame_count, label_count, w_enc, w_pred, b_joint, w_out, b_out)
        added = tuple((total + term for total, term in zip(grad_sums, grads_one)))
        return ((loss_sum + loss_one, added), None)
    (loss_sum, grads), unused_ys = lax.scan(one_utterance, (jnp.float32(0.0), initial), (enc, pred, labels, frame_len, label_len))
    return (loss_sum, grads)

def reference(enc, pred, labels, frame_len, label_len, w_enc, w_pred, b_joint, w_out, b_out):
    loss_sum, grads = local_sums(enc, pred, labels, frame_len, label_len, w_enc, w_pred, b_joint, w_out, b_out)
    param_count = sum((int(item.size) for item in grads))
    total_sq = jnp.float32(0.0)
    for item in grads:
        total_sq = total_sq + jnp.sum(item * item)
    scale = lax.rsqrt(total_sq / jnp.float32(param_count) + EPS)
    label_total = jnp.sum(label_len).astype(jnp.float32)
    return (grads[0] * scale, grads[1] * scale, grads[2] * scale, grads[3] * scale, grads[4] * scale, loss_sum / label_total)
```

```python
import functools

import jax
import jax.numpy as jnp
from jax import lax
from jax.experimental import pallas as pl
from jax.experimental.pallas import tpu as pltpu
from jax.sharding import PartitionSpec as P

NEG = -1e30
EPS = 1e-06
LANES = 128
AXES = ("dp", "rep")
WIDE = 1024
HALF = WIDE // 2
WIDE_BITS = 10
HALF_BITS = 9
VMEM_LIMIT = 60 * 1024 * 1024


def round_up(value, step):
    return (value + step - 1) // step * step


def log_add(a, b):
    return jnp.maximum(a, b) + jnp.log(1.0 + jnp.exp(-jnp.abs(a - b)))


def full_spec(shape):
    return pl.BlockSpec(shape, lambda *unused: (0,) * len(shape))


def forward_kernel(
    dims,
    labels_ref, frames_ref, counts_ref, core_ref,
    enc_ref, pred_ref, w_enc_ref, w_pred_ref, b_joint_ref, w_out_ref, b_out_ref,
    *refs,
):
    pieces = dims[4]
    out_refs = refs[:pieces]
    (
        hidden_ref, dlogits_ref, loss_ref, bias_ref,
        pred_proj_ref, hidden_t_ref, exp_ref, logit_ref, block_max_ref, max_ref, sum_ref, blank_ref, emit_ref,
        alpha_ref, beta_ref, even_ref, odd_ref, even_grad_ref, odd_grad_ref, copy_sem,
    ) = refs[pieces:]
    utterances, num_frames, count_labels, width = dims[:4]
    rows_one = num_frames * count_labels
    rows = utterances * rows_one
    block = pl.program_id(0)
    diagonals = num_frames + count_labels - 1
    padded = round_up(count_labels, 8)
    pred_stride = round_up(count_labels, 8)

    @pl.when(block == 0)
    def project():
        for b in range(utterances):
            pred_proj_ref[b * pred_stride : b * pred_stride + count_labels, :] = jnp.dot(
                pred_ref[b], w_pred_ref[...], preferred_element_type=jnp.float32
            ) + b_joint_ref[:, b_joint_ref.shape[1] - width :]
        for b in range(utterances):
            enc_proj = jnp.dot(enc_ref[b], w_enc_ref[...], preferred_element_type=jnp.float32)
            for u in range(count_labels):
                at = (b * count_labels + u) * num_frames
                row = pred_proj_ref[b * pred_stride + u : b * pred_stride + u + 1, :]
                hidden_ref[at : at + num_frames, :] = jnp.tanh(enc_proj + row).astype(jnp.bfloat16)
        for at in range(0, rows, LANES):
            size = min(LANES, rows - at)
            hidden_t_ref[0:width, at : at + size] = hidden_ref[at : at + size, :].T
        tail = hidden_t_ref.shape[0] - width
        hidden_t_ref[width:, :] = jnp.ones((tail, rows), jnp.bfloat16)
        max_ref[...] = jnp.full(max_ref.shape, NEG, jnp.float32)
        sum_ref[...] = jnp.zeros(sum_ref.shape, jnp.float32)
        bias_ref[...] = jnp.zeros(bias_ref.shape, jnp.float32)

    lane = lax.broadcasted_iota(jnp.int32, (16, LANES), 1)
    bias_row = b_out_ref[...]
    step = 6 * num_frames
    starts = list(range(0, rows, step))

    def exponentials(at, size):
        for r in range(at, at + size, 16):
            top = block_max_ref[r : r + 16, :]
            total = jnp.zeros((16, LANES), jnp.float32)
            for c in range(0, WIDE, LANES):
                value = jnp.exp(logit_ref[r : r + 16, c : c + LANES] - top)
                total = total + value
                exp_ref[r : r + 16, pl.ds(pl.multiple_of(block * WIDE + c, LANES), LANES)] = value.astype(jnp.bfloat16)
            mine = lane == block
            row_sum = jnp.sum(total, axis=1, keepdims=True)
            sum_ref[r : r + 16, :] = jnp.where(mine, row_sum, sum_ref[r : r + 16, :])
            max_ref[r : r + 16, :] = jnp.where(mine, top, max_ref[r : r + 16, :])

    before = None
    for at in starts:
        size = min(step, rows - at)
        logits = (
            jnp.dot(hidden_ref[at : at + size, :], w_out_ref[...], preferred_element_type=jnp.float32)
            + bias_row
        )
        logit_ref[at : at + size, :] = logits
        block_max_ref[at : at + size, :] = jnp.broadcast_to(
            jnp.max(logits, axis=1, keepdims=True), (size, LANES)
        )
        if before is not None:
            exponentials(*before)
        before = (at, size)
    exponentials(*before)

    lane_t = lax.broadcasted_iota(jnp.int32, (num_frames, LANES), 1)

    for b in range(utterances):
        for u in range(count_labels):
            label = labels_ref[b, u] if u < count_labels - 1 else jnp.int32(1)

            @pl.when((label >> WIDE_BITS) == block)
            def pick(b=b, u=u, label=label):
                at = (b * count_labels + u) * num_frames
                inner = label & (WIDE - 1)
                off = pl.multiple_of(inner & ~(LANES - 1), LANES)
                tile = logit_ref[at : at + num_frames, pl.ds(off, LANES)]
                hit = lane_t == (inner & (LANES - 1))
                value = jnp.sum(jnp.where(hit, tile, 0.0), axis=1, keepdims=True)
                emit_ref[at : at + num_frames, :] = jnp.broadcast_to(value, (num_frames, LANES))

    @pl.when(block == 0)
    def pick_blank():
        for at in range(0, rows, num_frames):
            tile = logit_ref[at : at + num_frames, 0:LANES]
            blank_ref[at : at + num_frames, :] = jnp.broadcast_to(
                tile[:, 0:1], (num_frames, LANES)
            )

    @pl.when(block == pl.num_programs(0) - 1)
    def finish():
        for at in range(0, rows, num_frames):
            here = slice(at, at + num_frames)
            tops = max_ref[here, :]
            top = jnp.max(tops, axis=1, keepdims=True)
            scaled = jnp.exp(tops - top)
            total = jnp.sum(sum_ref[here, :] * scaled, axis=1, keepdims=True)
            log_total = top + jnp.log(total)
            blank_ref[here, :] = blank_ref[here, :] - log_total
            emit_ref[here, :] = emit_ref[here, :] - log_total
            max_ref[here, :] = scaled / total

        u_ids = lax.broadcasted_iota(jnp.int32, (padded, LANES), 0)
        neg = jnp.full((padded, LANES), NEG, jnp.float32)
        base = [b * (diagonals + 1) * padded for b in range(utterances)]

        def at_diagonal(ref, b, d):
            return ref[pl.ds(b * rows_one + d, padded, stride=num_frames - 1), :]

        def shift_down(x):
            return jnp.where(u_ids == 0, NEG, pltpu.roll(x, 1, 0))

        def shift_up(x):
            return jnp.where(u_ids == padded - 1, NEG, pltpu.roll(x, padded - 1, 0))

        def below_of(b, t, beta_next):
            frames, count = frames_ref[b], counts_ref[b]
            terminal = jnp.where(u_ids == count, 0.0, NEG)
            return jnp.where(t == frames - 1, terminal, jnp.where(t >= frames, NEG, beta_next))

        def valid(t):
            return (t >= 0) & (t < num_frames) & (u_ids < count_labels)

        for b in range(utterances):
            beta_ref[base[b] + diagonals * padded : base[b] + (diagonals + 1) * padded, :] = neg

        def both_ways(i, carry):
            out = []
            for b in range(utterances):
                alpha, beta = carry[b]
                alpha_ref[pl.ds(pl.multiple_of(base[b] + i * padded, 8), padded), :] = alpha
                ok = valid(i - u_ids)
                blank = jnp.where(ok, at_diagonal(blank_ref, b, i), NEG)
                emit = jnp.where(ok, at_diagonal(emit_ref, b, i), NEG)
                ahead = i + 1 - u_ids
                alpha_new = log_add(alpha + blank, shift_down(alpha + emit))
                alpha_new = jnp.where((ahead >= 0) & (ahead < num_frames), alpha_new, NEG)

                d = diagonals - 1 - i
                t = d - u_ids
                ok = valid(t)
                blank = jnp.where(ok, at_diagonal(blank_ref, b, d), NEG)
                emit = jnp.where(ok, at_diagonal(emit_ref, b, d), NEG)
                beta_new = log_add(below_of(b, t, beta) + blank, shift_up(beta) + emit)
                live = (u_ids <= counts_ref[b]) & (t < frames_ref[b]) & (t >= 0)
                beta_new = jnp.where(live, beta_new, NEG)
                beta_ref[pl.ds(pl.multiple_of(base[b] + d * padded, 8), padded), :] = beta_new
                out.append((alpha_new, beta_new))
            return tuple(out)

        first = jnp.where(u_ids == 0, 0.0, NEG)
        lax.fori_loop(0, diagonals, both_ways, tuple((first, neg) for b in range(utterances)))

        log_totals = [beta_ref[base[b] : base[b] + 1, :] for b in range(utterances)]
        for b in range(utterances):
            loss_ref[b : b + 1, :] = -log_totals[b]

        def occupy(d, unused):
            for b in range(utterances):
                here = pl.ds(pl.multiple_of(base[b] + d * padded, 8), padded)
                after = pl.ds(pl.multiple_of(base[b] + (d + 1) * padded, 8), padded)
                alpha, beta_next = alpha_ref[here, :], beta_ref[after, :]
                t = d - u_ids
                ok = valid(t)
                blank = jnp.where(ok, at_diagonal(blank_ref, b, d), NEG)
                emit = jnp.where(ok, at_diagonal(emit_ref, b, d), NEG)
                alpha_ref[here, :] = jnp.exp(
                    alpha + blank + below_of(b, t, beta_next) - log_totals[b]
                )
                beta_ref[here, :] = jnp.exp(alpha + emit + shift_up(beta_next) - log_totals[b])
            return unused

        lax.fori_loop(0, diagonals, occupy, 0)

        for b in range(utterances):
            for u in range(count_labels):
                at = (b * count_labels + u) * num_frames
                here = slice(at, at + num_frames)
                cells = pl.ds(base[b] + u * (padded + 1), num_frames, stride=padded)
                blank_occ, emit_occ = alpha_ref[cells, :], beta_ref[cells, :]
                both = blank_occ + emit_occ
                max_ref[here, :] = max_ref[here, :] * both
                blank_ref[here, :] = jnp.exp(blank_ref[here, :]) * both - blank_occ
                emit_ref[here, :] = jnp.exp(emit_ref[here, :]) * both - emit_occ

        def columns(index):
            pair, kind, slot = index // 4, (index // 2) % 2, index % 2
            side = jnp.where(kind == 0, 1 - core_ref[0], core_ref[0])
            return 2 * (2 * pair + slot) + side

        def to_dlogits(index, target_ref):
            col = columns(index)
            blank_at = jnp.where(col == 0, 0, -1)
            for b in range(utterances):
                for u in range(count_labels):
                    at = (b * count_labels + u) * num_frames
                    here = slice(at, at + num_frames)
                    label = labels_ref[b, u] if u < count_labels - 1 else jnp.int32(1)
                    inner = label - col * HALF
                    weight = jnp.sum(
                        jnp.where(lane_t == col // 2, max_ref[here, :], 0.0), axis=1, keepdims=True
                    )
                    weight = jnp.broadcast_to(weight, (num_frames, LANES))
                    for c in range(0, HALF, LANES):
                        source = pl.ds(pl.multiple_of(col * HALF + c, LANES), LANES)
                        value = exp_ref[here, source].astype(jnp.float32) * weight
                        value = jnp.where(lane_t == inner - c, emit_ref[here, :], value)
                        if c == 0:
                            value = jnp.where(lane_t == blank_at, blank_ref[here, :], value)
                        target_ref[here, c : c + LANES] = value.astype(jnp.bfloat16)

        def dlogits_copy(index, source_ref):
            at = pl.ds(pl.multiple_of(columns(index) * HALF, HALF), HALF)
            return pltpu.make_async_copy(source_ref, dlogits_ref.at[:, at], copy_sem.at[index % 2])

        def grad_copy(index, source_ref, slot):
            return pltpu.make_async_copy(source_ref, out_refs[index], copy_sem.at[2 + slot])

        def to_grad(index, source_ref, grad_ref):
            grad = jnp.dot(hidden_t_ref[...], source_ref[...], preferred_element_type=jnp.float32)
            at = pl.ds(pl.multiple_of(columns(index) * HALF, HALF), HALF)
            bias_ref[:, at] = grad[width : width + 8, :]
            grad_ref[...] = grad[0:width, :]

        to_dlogits(jnp.int32(0), even_ref)

        def two_pieces(it, unused):
            first, second = 2 * it, 2 * it + 1
            following = jnp.minimum(first + 2, pieces - 1)

            @pl.when(it > 0)
            def drain():
                dlogits_copy(second - 2, odd_ref).wait()
                grad_copy(0, even_grad_ref, 0).wait()
                grad_copy(1, odd_grad_ref, 1).wait()

            dlogits_copy(first, even_ref).start()
            to_grad(first, even_ref, even_grad_ref)
            to_dlogits(second, odd_ref)
            for k in range(0, pieces, 2):

                @pl.when(first == k)
                def send_even(k=k):
                    grad_copy(k, even_grad_ref, 0).start()

            dlogits_copy(second, odd_ref).start()
            dlogits_copy(first, even_ref).wait()
            to_grad(second, odd_ref, odd_grad_ref)
            to_dlogits(following, even_ref)
            for k in range(1, pieces, 2):

                @pl.when(second == k)
                def send_odd(k=k):
                    grad_copy(k, odd_grad_ref, 1).start()

            return unused

        lax.fori_loop(0, pieces // 2, two_pieces, 0)
        dlogits_copy(pieces - 1, odd_ref).wait()
        grad_copy(pieces - 2, even_grad_ref, 0).wait()
        grad_copy(pieces - 1, odd_grad_ref, 1).wait()


def forward(core, enc, pred, labels, frame_len, label_len, w_enc, w_pred, b_joint, w_out, b_out):
    utterances, num_frames, features = enc.shape
    count_labels = pred.shape[1]
    width, vocab = w_out.shape
    rows = utterances * num_frames * count_labels
    padded = round_up(count_labels, 8)
    diagonals = num_frames + count_labels - 1
    pieces = vocab // HALF
    biases = jnp.concatenate([b_out, b_joint]).astype(jnp.float32).reshape(1, -1)
    tall = round_up(rows + (padded - count_labels) * (num_frames - 1) + num_frames, 8)
    grid_spec = pltpu.PrefetchScalarGridSpec(
        num_scalar_prefetch=4,
        grid=(vocab // WIDE,),
        in_specs=[
            full_spec(enc.shape), full_spec(pred.shape), full_spec(w_enc.shape), full_spec(w_pred.shape),
            full_spec((1, vocab + width)),
            pl.BlockSpec((width, WIDE), lambda j, *unused: (0, j)),
            pl.BlockSpec((1, WIDE), lambda j, *unused: (0, j)),
        ],
        out_specs=[pl.BlockSpec(memory_space=pl.ANY) for piece in range(pieces)]
        + [
            full_spec((rows, width)), pl.BlockSpec(memory_space=pl.ANY),
            full_spec((utterances, LANES)), full_spec((8, vocab)),
        ],
        scratch_shapes=[
            pltpu.VMEM((utterances * padded, width), jnp.float32),
            pltpu.VMEM((width + 16, rows), jnp.bfloat16),
            pltpu.VMEM((rows, vocab), jnp.bfloat16),
            pltpu.VMEM((rows, WIDE), jnp.float32),
            pltpu.VMEM((rows, LANES), jnp.float32),
            pltpu.VMEM((rows, LANES), jnp.float32),
            pltpu.VMEM((rows, LANES), jnp.float32),
            pltpu.VMEM((tall, LANES), jnp.float32),
            pltpu.VMEM((tall, LANES), jnp.float32),
            pltpu.VMEM((utterances * (diagonals + 1) * padded, LANES), jnp.float32),
            pltpu.VMEM((utterances * (diagonals + 1) * padded, LANES), jnp.float32),
            pltpu.VMEM((rows, HALF), jnp.bfloat16),
            pltpu.VMEM((rows, HALF), jnp.bfloat16),
            pltpu.VMEM((width, HALF), jnp.float32),
            pltpu.VMEM((width, HALF), jnp.float32),
            pltpu.SemaphoreType.DMA((4,)),
        ],
    )
    outs = pl.pallas_call(
        functools.partial(forward_kernel, (utterances, num_frames, count_labels, width, pieces)),
        grid_spec=grid_spec,
        out_shape=[jax.ShapeDtypeStruct((width, HALF), jnp.float32) for piece in range(pieces)]
        + [
            jax.ShapeDtypeStruct((rows, width), jnp.bfloat16),
            jax.ShapeDtypeStruct((rows, vocab), jnp.bfloat16),
            jax.ShapeDtypeStruct((utterances, LANES), jnp.float32),
            jax.ShapeDtypeStruct((8, vocab), jnp.float32),
        ],
        compiler_params=pltpu.CompilerParams(
            dimension_semantics=("arbitrary",), vmem_limit_bytes=VMEM_LIMIT
        ),
        name="forward",
    )(labels, frame_len, label_len, core.reshape(1), enc, pred, w_enc, w_pred, biases, w_out, biases)
    return (outs[:pieces], *outs[pieces:])


def grad_in_kernel(
    dims, enc_ref, pred_ref, hidden_ref, dlogits_ref, w_out_ref, grad_ref, bias_ref,
    total_ref, d_enc_ref, d_pred_ref, pred_pad_ref,
):
    utterances, num_frames, count_labels, width = dims
    features = enc_ref.shape[2]
    pred_stride = round_up(count_labels, 16)
    block = pl.program_id(0)

    @pl.when(block == 0)
    def clear():
        total_ref[...] = jnp.zeros(total_ref.shape, jnp.float32)

    total_ref[...] += lax.dot_general(
        dlogits_ref[...], w_out_ref[...], (((1,), (1,)), ((), ())), preferred_element_type=jnp.float32
    )

    @pl.when(block == pl.num_programs(0) - 1)
    def finish():
        d_pred_ref[...] = jnp.zeros(d_pred_ref.shape, jnp.float32)
        pred_pad_ref[...] = jnp.zeros(pred_pad_ref.shape, jnp.bfloat16)
        for b in range(utterances):
            pred_pad_ref[b * pred_stride : b * pred_stride + count_labels, :] = pred_ref[b]
            d_enc = jnp.zeros((num_frames, width), jnp.float32)
            for u in range(count_labels):
                at = (b * count_labels + u) * num_frames
                hidden = hidden_ref[at : at + num_frames, :].astype(jnp.float32)
                d_pre = total_ref[at : at + num_frames, :] * (1.0 - hidden * hidden)
                d_enc = d_enc + d_pre
                d_pred_ref[b * pred_stride + u : b * pred_stride + u + 1, :] = jnp.sum(
                    d_pre, axis=0, keepdims=True
                )
            d_enc_ref[b * num_frames : (b + 1) * num_frames, :] = d_enc.astype(jnp.bfloat16)
        d_pred = d_pred_ref[...].astype(jnp.bfloat16)
        contract = (((0,), (0,)), ((), ()))
        enc_all = jnp.concatenate([enc_ref[b] for b in range(utterances)], axis=0)
        grad_ref[0:features, :] = lax.dot_general(
            enc_all, d_enc_ref[...], contract, preferred_element_type=jnp.float32
        )
        grad_ref[features:, :] = lax.dot_general(
            pred_pad_ref[...], d_pred, contract, preferred_element_type=jnp.float32
        )
        bias = jnp.sum(d_pred.astype(jnp.float32), axis=0, keepdims=True)
        bias_ref[...] = jnp.broadcast_to(bias, bias_ref.shape)


def grad_in(dims, enc, pred, hidden, dlogits, w_out):
    utterances, num_frames, count_labels, width = dims
    rows = utterances * num_frames * count_labels
    vocab = w_out.shape[1]
    features, more = enc.shape[2], pred.shape[2]
    pred_rows = utterances * round_up(count_labels, 16)
    return pl.pallas_call(
        functools.partial(grad_in_kernel, dims),
        grid=(vocab // WIDE,),
        in_specs=[
            full_spec(enc.shape), full_spec(pred.shape), full_spec(hidden.shape),
            pl.BlockSpec((rows, WIDE), lambda i: (0, i)),
            pl.BlockSpec((width, WIDE), lambda i: (0, i)),
        ],
        out_specs=[full_spec((features + more, width)), full_spec((8, width))],
        out_shape=[
            jax.ShapeDtypeStruct((features + more, width), jnp.float32),
            jax.ShapeDtypeStruct((8, width), jnp.float32),
        ],
        scratch_shapes=[
            pltpu.VMEM((rows, width), jnp.float32),
            pltpu.VMEM((utterances * num_frames, width), jnp.bfloat16),
            pltpu.VMEM((pred_rows, width), jnp.float32),
            pltpu.VMEM((pred_rows, more), jnp.bfloat16),
        ],
        cost_estimate=pl.CostEstimate(
            flops=2 * rows * width * vocab, bytes_accessed=rows * vocab * 2, transcendentals=0
        ),
        compiler_params=pltpu.CompilerParams(
            dimension_semantics=("arbitrary",), vmem_limit_bytes=VMEM_LIMIT
        ),
        name="grad_in",
    )(enc, pred, hidden, dlogits, w_out)


def place_kernel(chunk, first, *refs):
    core_ref, scale_ref, own_ref, other_ref = refs[:4]
    out_ref = refs[-1]
    scale = scale_ref[0]
    own, other = own_ref[...] * scale, other_ref[...] * scale
    low = core_ref[0] == 0
    out_ref[:, 0:HALF] = jnp.where(low, own, other)
    out_ref[:, HALF:] = jnp.where(low, other, own)


def place(chunk, core, scale, own, other, target, vocab):
    width = own.shape[0]
    tall = width // 4
    part = pl.BlockSpec((tall, HALF), lambda i, *unused: (i, 0))
    operands = [core.reshape(1), scale.reshape(1), own, other]
    in_specs = [part, part]
    aliases = {}
    if target is not None:
        operands.append(target)
        in_specs.append(pl.BlockSpec(memory_space=pl.ANY))
        aliases = {4: 0}
    return pl.pallas_call(
        functools.partial(place_kernel, chunk, target is None),
        grid_spec=pltpu.PrefetchScalarGridSpec(
            num_scalar_prefetch=2,
            grid=(width // tall,),
            in_specs=in_specs,
            out_specs=pl.BlockSpec((tall, WIDE), lambda i, *unused: (i, chunk)),
        ),
        out_shape=jax.ShapeDtypeStruct((width, vocab), jnp.float32),
        input_output_aliases=aliases,
        compiler_params=pltpu.CompilerParams(dimension_semantics=("arbitrary",)),
        name="place",
    )(*operands)


def exchange(x, bit, devices):
    return lax.ppermute(x, AXES, [(i, i ^ (1 << bit)) for i in range(devices)])


def butterfly(x, devices):
    bit = 0
    while 1 << bit < devices:
        x = x + exchange(x, bit, devices)
        bit += 1
    return x


def scatter_steps(cur, order, me, devices):
    for bit in order:
        mine = (me >> bit) & 1
        half = cur.shape[0] // 2
        send = lax.dynamic_slice_in_dim(cur, (1 - mine) * half, half, 0)
        keep = lax.dynamic_slice_in_dim(cur, mine * half, half, 0)
        cur = keep + exchange(send, bit, devices)
        yield cur


def gather_steps(cur, order, me, devices):
    for bit in reversed(order):
        mine = (me >> bit) & 1
        other = exchange(cur, bit, devices)
        cur = jnp.where(
            mine == 1, jnp.concatenate([other, cur], 0), jnp.concatenate([cur, other], 0)
        )
        yield cur


def drive(steps, outs):
    live = list(range(len(steps)))
    while live:
        for i in list(live):
            try:
                outs[i] = next(steps[i])
            except StopIteration:
                live.remove(i)
    return outs


def squares(items):
    return sum(jnp.sum(item * item) for item in items)


def per_device(devices, enc, pred, labels, frame_len, label_len, w_enc, w_pred, b_joint, w_out, b_out):
    utterances, num_frames, features = enc.shape
    count_labels = pred.shape[1]
    width, vocab = w_out.shape
    dims = (utterances, num_frames, count_labels, width)
    bits = devices.bit_length() - 1
    me = lax.axis_index(AXES)
    core = me & 1
    rest = list(range(1, bits))
    swapped = rest[1:2] + rest[:1] + rest[2:]
    turned = rest[2:] + rest[:2]

    grads, hidden, dlogits, loss, bias = forward(
        core, enc, pred, labels, frame_len, label_len, w_enc, w_pred, b_joint, w_out, b_out
    )
    chunks = vocab // WIDE
    totals = []
    for chunk in range(chunks):
        at = 4 * (chunk // 2) + chunk % 2
        totals.append(grads[at + 2] + exchange(grads[at], 0, devices))
    joint, joint_bias = grad_in(dims, enc, pred, hidden, dlogits, w_out)
    half = joint.shape[0] // 2
    joint_sent = lax.dynamic_slice_in_dim(joint, (1 - core) * half, half, 0)
    joint_kept = lax.dynamic_slice_in_dim(joint, core * half, half, 0)
    totals.append(joint_kept + exchange(joint_sent, 0, devices))

    small = jnp.concatenate([
        bias[0], joint_bias[0],
        jnp.sum(loss[:, 0]).reshape(1), jnp.sum(label_len).astype(jnp.float32).reshape(1),
    ])
    small_size = small.shape[0]
    small = jnp.pad(small, (0, round_up(small_size, 1024) - small_size)).reshape(-1, LANES)
    small = butterfly(small, devices).reshape(-1)

    orders = [rest if k % 2 == 0 else swapped for k in range(chunks)] + [turned]
    owned = drive([scatter_steps(t, o, me, devices) for t, o in zip(totals, orders)], list(totals))
    partial_sq = squares(owned)
    param_count = jnp.float32(w_enc.size + w_pred.size + w_out.size + b_out.size + b_joint.size)
    total_sq = butterfly(jnp.full((8, LANES), partial_sq), devices)[0, 0]
    total_sq = total_sq + squares([small[: vocab + width]])
    scale = lax.rsqrt(total_sq / param_count + EPS)

    whole = drive([gather_steps(t, o, me, devices) for t, o in zip(owned, orders)], list(owned))
    others = [exchange(t, 0, devices) for t in whole]
    step_out = None
    for chunk in range(chunks):
        step_out = place(chunk, core, scale, whole[chunk], others[chunk], step_out, vocab)
    low, high = jnp.where(core == 0, whole[-1], others[-1]), jnp.where(core == 0, others[-1], whole[-1])
    return (
        low * scale, high * scale, step_out,
        small[:vocab] * scale, small[vocab : vocab + width] * scale,
        small[vocab + width] / small[vocab + width + 1],
    )


def solution(mesh):
    devices = mesh.shape["dp"] * mesh.shape["rep"]
    both = P(AXES)
    return jax.shard_map(
        functools.partial(per_device, devices),
        mesh=mesh,
        in_specs=(both, both, both, both, both, P(), P(), P(), P(), P()),
        out_specs=(P(),) * 6,
        check_vma=False,
    )
```
